32 devices in a mesh: grp: 2 (over y), lat: 4 (over z), lay: 4 (over x, core).
Axes of the slice: x: 2, y: 2, z: 4, core: 2. Of those that a mesh axis runs over, the one named last changes fastest.
Arguments:
- acts: bfloat16 [128, 4, 1280], P(('grp', 'lat'), 'lay'), parts along dimension 0, may hold values from -6 to 6
- w_enc: bfloat16 [4, 1280, 1536], P('lay', None, 'lat'), may hold values from -0.078125 to 0.078125
- w_dec: bfloat16 [1536, 4, 1280], P('lat', 'lay'), may hold values from -0.15625 to 0.15625
- b_enc: float32 [1536], P('lat'), may hold values from -3 to 3
- b_dec: float32 [4, 1280], P('lay'), may hold values from -3 to 3
Outputs:
- lat_grad: bfloat16 [128, 1536], P('grp', 'lat'), parts along dimension 0
- enc_grad: bfloat16 [8, 1280, 1536], P(('grp', 'lay'), None, 'lat'), parts along dimension 0
- dec_grad: bfloat16 [1536, 8, 1280], P('lat', ('grp', 'lay')), parts along dimension 1
The draws below stay inside these ranges and needn't reach their ends.
There are 2 independent parts, one for each index of `grp`. The reference program is written for one: setup_inputs(seed, part) draws one part's arguments, and reference() takes and returns one part's arrays. A program takes and returns all parts, laid end to end along the dimension named above; an argument that names none is the same for every part. Nothing has to cross between parts.
All inputs are finite; a program needn't handle non-finite values.
Results may differ from the reference program's by a relative error of at most 0.023.
Values may be sent and summed in bfloat16 or wider, within the bound.
A program may use at most 64 MiB of HBM per device.

```python
import jax
import jax.numpy as jnp

D = 1280
LATENTS = 1536
LAYERS = 4
ROWS = 64


def levels(stream_key, extent, pieces, least, top_value):
    def one(dim, parts):
        heights = jax.random.uniform(jax.random.fold_in(jax.random.fold_in(stream_key, 6), dim), (parts,), jnp.float32, least / len(pieces), top_value / len(pieces))
        return jnp.repeat(jnp.exp(heights), extent[dim] // parts).reshape((-1,) + (1,) * (len(extent) - dim - 1))

    level = one(*pieces[0])
    for cut in pieces[1:]:
        level = level * one(*cut)
    return level


def noise(key, dims, width, most, shards=(), held_as=jnp.bfloat16):
    array = width * jax.random.normal(key, dims, jnp.float32)
    if shards:
        array = array * levels(key, dims, shards, -0.22, 0.18)
    return jnp.clip(array, -most, most).astype(held_as)


def setup_inputs(seed: int = 0, part: int = 0) -> dict:
    streams_of = jax.random.split(jax.random.key(seed), 6)
    part_splits = jax.random.split(jax.random.fold_in(streams_of[5], part), 6)
    return {
        "acts": noise(part_splits[0], (ROWS, LAYERS, D), 1.0, 6.0, ((0, 4), (1, 4))),
        "w_enc": noise(streams_of[1], (LAYERS, D, LATENTS), (LAYERS * D) ** -0.5, 0.078125, ((0, 4), (2, 4))),
        "w_dec": noise(streams_of[2], (LATENTS, LAYERS, D), LATENTS ** -0.5, 0.15625, ((0, 4), (1, 4))),
        "b_enc": noise(streams_of[3], (LATENTS,), 0.5, 3.0, ((0, 4),), jnp.float32),
        "b_dec": noise(streams_of[4], (LAYERS, D), 0.5, 3.0, ((0, 4),), jnp.float32),
    }


def reference(acts, w_enc, w_dec, b_enc, b_dec):
    x32 = acts.astype(jnp.float32)
    pre = jnp.einsum("bld,ldm->bm", x32, w_enc.astype(jnp.float32)) + b_enc[None, :]
    code = (jax.nn.softplus(4.0 * pre) / 4.0).astype(jnp.bfloat16)
    slope = jax.nn.sigmoid(4.0 * pre)
    recon = jnp.einsum("bm,mld->bld", code.astype(jnp.float32), w_dec.astype(jnp.float32))
    err = (recon + b_dec[None, :, :] - x32).astype(jnp.bfloat16)
    back = jnp.einsum("bld,mld->bm", err.astype(jnp.float32), w_dec.astype(jnp.float32))
    lat_grad = (back * slope).astype(jnp.bfloat16)
    enc_grad = jnp.einsum("bld,bm->ldm", x32, lat_grad.astype(jnp.float32)).astype(jnp.bfloat16)
    dec_grad = jnp.einsum("bm,bld->mld", code.astype(jnp.float32), err.astype(jnp.float32)).astype(jnp.bfloat16)
    return lat_grad, enc_grad, dec_grad
```

```python
import functools

import jax
import jax.numpy as jnp
from jax import lax
from jax.experimental import pallas as pl
from jax.experimental.pallas import tpu as pltpu
from jax.sharding import PartitionSpec as P

MESH = pl.DeviceIdType.MESH
F32, BF16 = jnp.float32, jnp.bfloat16
NT = (((1,), (1,)), ((), ()))


def step(
    n_lat, n_lay, acts_hbm, wenc_hbm, wdec_hbm, benc_ref, bdec_ref, lat_out, enc_out, dec_out,
    acts_all, wenc, wdec, pre_buf, back_buf, rec_mine, rec_buf, err_all,
    load, acts_s, acts_r, pre_s, pre_r, rec_s, rec_r, err_s, err_r, back_s, back_r,
):
    z, l = lax.axis_index("lat"), lax.axis_index("lay")
    row_dev, wide = acts_all.shape[1:]
    rows, lat_dev = n_lat * row_dev, wenc.shape[1]

    load_acts = pltpu.make_async_copy(acts_hbm, acts_all.at[z], load.at[0])
    load_enc = pltpu.make_async_copy(wenc_hbm, wenc, load.at[1])
    load_dec = pltpu.make_async_copy(wdec_hbm, wdec, load.at[2])
    load_acts.start()
    load_enc.start()
    load_dec.start()

    def lat_peer(k):
        return {"lat": lax.rem(z + k, n_lat)}

    def lay_peer(k):
        return {"lay": lax.rem(l + k, n_lay)}

    barrier = pltpu.get_barrier_semaphore()
    for k in range(1, n_lat):
        pl.semaphore_signal(barrier, inc=1, device_id=lat_peer(k), device_id_type=MESH)
    for k in range(1, n_lay):
        pl.semaphore_signal(barrier, inc=1, device_id=lay_peer(k), device_id_type=MESH)
    pl.semaphore_wait(barrier, n_lat + n_lay - 2)

    def send(src, dst, send_sem, recv_sem, peer):
        copy = pltpu.make_async_remote_copy(
            src_ref=src, dst_ref=dst, send_sem=send_sem, recv_sem=recv_sem,
            device_id=peer, device_id_type=MESH,
        )
        copy.start()
        return copy

    started = []

    def to_lat(buf, sent, received, src=None):
        copies = []
        for k in range(1, n_lat):
            block = buf.at[z] if src is None else src.at[lax.rem(z + k, n_lat)]
            copies.append(send(block, buf.at[z], sent.at[k], received.at[k], lat_peer(k)))
        started.extend(copies)
        return copies

    def to_lay(buf, sent, received):
        copies = [
            send(buf.at[l], buf.at[l], sent.at[k], received.at[k], lay_peer(k))
            for k in range(1, n_lay)
        ]
        started.extend(copies)
        return copies

    def total(buf):
        whole = buf[0].astype(F32)
        for i in range(1, n_lay):
            whole += buf[i].astype(F32)
        return whole

    load_acts.wait()
    copies = to_lat(acts_all, acts_s, acts_r)
    load_enc.wait()
    for copy in copies:
        copy.wait_recv()
    acts = acts_all[...].reshape(rows, wide)
    pre_buf[l] = jnp.dot(acts, wenc[...], preferred_element_type=F32).astype(BF16)
    copies = to_lay(pre_buf, pre_s, pre_r)
    load_dec.wait()
    for copy in copies:
        copy.wait_recv()
    x = 4.0 * (total(pre_buf) + benc_ref[...].reshape(1, lat_dev))
    e = jnp.exp(-jnp.abs(x))
    code = (0.25 * (jnp.maximum(x, 0.0) + jnp.log1p(e))).astype(BF16)
    rec_mine[...] = (
        jnp.dot(code, wdec[...], preferred_element_type=F32).astype(BF16).reshape(rec_mine.shape)
    )
    copies = to_lat(rec_buf, rec_s, rec_r, rec_mine)
    slope = jnp.where(x >= 0.0, 1.0, e) / (1.0 + e)
    acts_t = acts.astype(F32).T.astype(BF16)
    code_t = code.astype(F32).T.astype(BF16)
    err = bdec_ref[...] - acts_all[z].astype(F32) + rec_mine[z].astype(F32)
    for k, copy in enumerate(copies, 1):
        copy.wait_recv()
        err += rec_buf[lax.rem(z + n_lat - k, n_lat)].astype(F32)
    err_all[z] = err.astype(BF16)
    copies = to_lat(err_all, err_s, err_r)
    for copy in copies:
        copy.wait_recv()
    errs = err_all[...].reshape(rows, wide)
    back_buf[l] = lax.dot_general(errs, wdec[...], NT, preferred_element_type=F32).astype(BF16)
    copies = to_lay(back_buf, back_s, back_r)
    dec_out[...] = jnp.dot(code_t, errs, preferred_element_type=F32).astype(BF16)
    for copy in copies:
        copy.wait_recv()
    lat_grad = (total(back_buf) * slope).astype(BF16)
    lat_out[...] = lat_grad
    enc_out[...] = jnp.dot(acts_t, lat_grad, preferred_element_type=F32).astype(BF16)
    for copy in started:
        copy.wait_send()


def solution(mesh):
    n_lat, n_lay = mesh.shape["lat"], mesh.shape["lay"]

    def on_device(acts, w_enc, w_dec, b_enc, b_dec):
        row_dev, lay_dev, width = acts.shape
        lat_dev = w_enc.shape[2]
        wide, rows = lay_dev * width, n_lat * row_dev
        hbm = pl.BlockSpec(memory_space=pltpu.HBM)
        vmem = pl.BlockSpec(memory_space=pltpu.VMEM)
        dma = pltpu.SemaphoreType.DMA
        lat_grad, enc_grad, dec_grad = pl.pallas_call(
            functools.partial(step, n_lat, n_lay),
            out_shape=[
                jax.ShapeDtypeStruct((rows, lat_dev), BF16),
                jax.ShapeDtypeStruct((wide, lat_dev), BF16),
                jax.ShapeDtypeStruct((lat_dev, wide), BF16),
            ],
            in_specs=[hbm, hbm, hbm, vmem, vmem],
            out_specs=[vmem, vmem, vmem],
            scratch_shapes=[
                pltpu.VMEM((n_lat, row_dev, wide), BF16),
                pltpu.VMEM((wide, lat_dev), BF16),
                pltpu.VMEM((lat_dev, wide), BF16),
                pltpu.VMEM((n_lay, rows, lat_dev), BF16),
                pltpu.VMEM((n_lay, rows, lat_dev), BF16),
                pltpu.VMEM((n_lat, row_dev, wide), BF16),
                pltpu.VMEM((n_lat, row_dev, wide), BF16),
                pltpu.VMEM((n_lat, row_dev, wide), BF16),
                dma((3,)),
                dma((n_lat,)), dma((n_lat,)),
                dma((n_lay,)), dma((n_lay,)),
                dma((n_lat,)), dma((n_lat,)),
                dma((n_lat,)), dma((n_lat,)),
                dma((n_lay,)), dma((n_lay,)),
            ],
            compiler_params=pltpu.CompilerParams(collective_id=0, has_side_effects=True),
            cost_estimate=pl.CostEstimate(
                flops=10 * rows * wide * lat_dev,
                bytes_accessed=8 * wide * lat_dev,
                transcendentals=0,
            ),
        )(
            acts.reshape(row_dev, wide),
            w_enc.reshape(wide, lat_dev),
            w_dec.reshape(lat_dev, wide),
            b_enc,
            b_dec.reshape(1, wide),
        )
        return (
            lat_grad,
            enc_grad.reshape(lay_dev, width, lat_dev),
            dec_grad.reshape(lat_dev, lay_dev, width),
        )

    in_specs = (
        P(("grp", "lat"), "lay", None),
        P("lay", None, "lat"),
        P("lat", "lay", None),
        P("lat"),
        P("lay", None),
    )
    out_specs = (P("grp", "lat"), P(("grp", "lay"), None, "lat"), P("lat", ("grp", "lay"), None))
    return jax.shard_map(
        on_device, mesh=mesh, in_specs=in_specs, out_specs=out_specs, check_vma=False
    )
```

```python
import functools

import jax
import jax.numpy as jnp
from jax import lax
from jax.experimental import pallas as pl
from jax.experimental.pallas import tpu as pltpu
from jax.sharding import PartitionSpec as P

MESH = pl.DeviceIdType.MESH
F32, BF16 = jnp.float32, jnp.bfloat16


def flip(v, j):
    out, bit = v, 1
    while bit <= j:
        if j & bit:
            out = out + bit * (1 - 2 * lax.rem(lax.div(v, bit), 2))
        bit *= 2
    return out


def step(
    n_lat, n_lay, groups, acts_hbm, wenc_hbm, wdec_hbm, benc_ref, bdec_ref,
    lat_out, acts_t, dec_out,
    acts_all, wenc, wdec, wdec_t, pre_buf, back_buf, rec_mine, rec_buf, err_all, code_all, slope,
    load, acts_s, acts_r, pre_s, pre_r, rec_s, rec_r, err_s, err_r, back_s, back_r,
):
    z, l = lax.axis_index("lat"), lax.axis_index("lay")
    row_dev, wide = acts_all.shape[1:]
    rows, lat_dev = n_lat * row_dev, wenc.shape[1]
    size = n_lat // groups
    part = size * row_dev

    load_acts = pltpu.make_async_copy(acts_hbm, acts_all.at[z], load.at[0])
    load_enc = pltpu.make_async_copy(wenc_hbm, wenc, load.at[1])
    load_dec = pltpu.make_async_copy(wdec_hbm, wdec, load.at[2])
    load_acts.start()
    load_enc.start()
    load_dec.start()

    if groups > 1:
        dest = source = lambda j: flip(z, j)
    else:
        dest = lambda j: lax.rem(z + j, n_lat)
        source = lambda j: lax.rem(z + n_lat - j, n_lat)
    group = [flip(lax.div(z, size), g) if groups > 1 else 0 for g in range(groups)]

    def lay_peer(k):
        return {"lay": lax.rem(l + k, n_lay)}

    barrier = pltpu.get_barrier_semaphore()
    for j in reversed(range(1, n_lat)):
        pl.semaphore_signal(
            barrier, inc=1, device_id={"lat": dest(j)}, device_id_type=MESH
        )
    for k in range(1, n_lay):
        pl.semaphore_signal(barrier, inc=1, device_id=lay_peer(k), device_id_type=MESH)
    pl.semaphore_wait(barrier, n_lat + n_lay - 2)

    started = []

    def send(src, dst, send_sem, recv_sem, peer):
        copy = pltpu.make_async_remote_copy(
            src_ref=src, dst_ref=dst, send_sem=send_sem, recv_sem=recv_sem,
            device_id=peer, device_id_type=MESH,
        )
        copy.start()
        started.append(copy)
        return copy

    def to_lat(buf, sent, received):
        return {
            j: send(buf.at[z], buf.at[z], sent.at[j], received.at[j], {"lat": dest(j)})
            for j in reversed(range(1, n_lat))
        }

    def to_lay(buf, g, sent, received):
        block = buf.at[l, group[g]]
        return [
            send(block, block, sent.at[g, k], received.at[g, k], lay_peer(k))
            for k in range(1, n_lay)
        ]

    def arrive(copies, g):
        for j in range(g * size, (g + 1) * size):
            if j:
                copies[j].wait_recv()

    def rows_of(buf, g):
        return buf[pl.ds(group[g] * size, size)].reshape(part, wide)

    def total(buf, g):
        whole = buf[0, group[g]].astype(F32)
        for i in range(1, n_lay):
            whole += buf[i, group[g]].astype(F32)
        return whole

    load_acts.wait()
    acts_copies = to_lat(acts_all, acts_s, acts_r)
    load_enc.wait()
    pre_copies, rec_copies = {}, {}

    def encode(g):
        arrive(acts_copies, g)
        pre = jnp.dot(rows_of(acts_all, g), wenc[...], preferred_element_type=F32)
        pre_buf[l, group[g]] = pre.astype(BF16)
        pre_copies[g] = to_lay(pre_buf, g, pre_s, pre_r)

    def decode(g):
        for copy in pre_copies[g]:
            copy.wait_recv()
        x = 4.0 * (total(pre_buf, g) + benc_ref[...].reshape(1, lat_dev))
        e = jnp.exp(-jnp.abs(x))
        code = (0.25 * (jnp.maximum(x, 0.0) + jnp.log1p(e))).astype(BF16)
        rec = jnp.dot(code, wdec[...], preferred_element_type=F32).astype(BF16)
        rec_mine[pl.ds(group[g] * size, size)] = rec.reshape(size, row_dev, wide)
        for j in range(g * size, (g + 1) * size):
            if j:
                rec_copies[j] = send(
                    rec_mine.at[dest(j)], rec_buf.at[z], rec_s.at[j], rec_r.at[j],
                    {"lat": dest(j)},
                )
        code_all[group[g]] = code
        slope[group[g]] = jnp.where(x >= 0.0, 1.0, e) / (1.0 + e)

    for g in range(groups):
        if g == groups - 1 and g:
            decode(0)
        encode(g)
        if g == 0:
            load_dec.wait()
            wdec_t[...] = wdec[...].astype(F32).T.astype(BF16)
    for g in range(1 if groups > 1 else 0, groups):
        decode(g)
    acts_t[...] = acts_all[...].reshape(rows, wide).astype(F32).T.astype(BF16)
    code_t = code_all[...].reshape(rows, lat_dev).astype(F32).T.astype(BF16)
    err = bdec_ref[...] - acts_all[z].astype(F32) + rec_mine[z].astype(F32)
    for j in range(1, n_lat):
        rec_copies[j].wait_recv()
        err += rec_buf[source(j)].astype(F32)
    err_all[z] = err.astype(BF16)
    err_copies = to_lat(err_all, err_s, err_r)
    back_copies = {}
    for g in range(groups):
        arrive(err_copies, g)
        back = jnp.dot(rows_of(err_all, g), wdec_t[...], preferred_element_type=F32)
        back_buf[l, group[g]] = back.astype(BF16)
        back_copies[g] = to_lay(back_buf, g, back_s, back_r)
    errs = err_all[...].reshape(rows, wide)
    dec_out[...] = jnp.dot(code_t, errs, preferred_element_type=F32).astype(BF16)
    for g in range(groups):
        for copy in back_copies[g]:
            copy.wait_recv()
        lat_out[group[g]] = (total(back_buf, g) * slope[group[g]]).astype(BF16)
    for copy in started:
        copy.wait_send()


def finish(chunks, lat, acts_t, dec, lat_hbm, enc_hbm, dec_hbm, enc, sems):
    rows, lat_dev = lat.shape[0] * lat.shape[1], lat.shape[2]
    copies = [
        pltpu.make_async_copy(dec, dec_hbm, sems.at[0]),
        pltpu.make_async_copy(lat, lat_hbm, sems.at[1]),
    ]
    for copy in copies:
        copy.start()
    grad = lat[...].reshape(rows, lat_dev)
    tall = enc.shape[0] // chunks
    for c in range(chunks):
        cut = pl.ds(c * tall, tall)
        enc[cut] = jnp.dot(acts_t[cut], grad, preferred_element_type=F32).astype(BF16)
        copy = pltpu.make_async_copy(enc.at[cut], enc_hbm.at[cut], sems.at[2 + c])
        copy.start()
        copies.append(copy)
    for copy in copies:
        copy.wait()


def solution(mesh):
    n_lat, n_lay = mesh.shape["lat"], mesh.shape["lay"]

    def on_device(acts, w_enc, w_dec, b_enc, b_dec):
        row_dev, lay_dev, width = acts.shape
        lat_dev = w_enc.shape[2]
        wide, rows = lay_dev * width, n_lat * row_dev
        hbm = pl.BlockSpec(memory_space=pltpu.HBM)
        vmem = pl.BlockSpec(memory_space=pltpu.VMEM)
        dma = pltpu.SemaphoreType.DMA
        groups = 4 if n_lat & (n_lat - 1) == 0 and n_lat % 4 == 0 else 1
        part = rows // groups
        chunks = 5 if wide % 80 == 0 else 1
        lat_part, acts_t, dec_part = pl.pallas_call(
            functools.partial(step, n_lat, n_lay, groups),
            out_shape=[
                pltpu.VMEM((groups, part, lat_dev), BF16),
                pltpu.VMEM((wide, rows), BF16),
                pltpu.VMEM((lat_dev, wide), BF16),
            ],
            in_specs=[hbm, hbm, hbm, vmem, vmem],
            out_specs=[vmem, vmem, vmem],
            scratch_shapes=[
                pltpu.VMEM((n_lat, row_dev, wide), BF16),
                pltpu.VMEM((wide, lat_dev), BF16),
                pltpu.VMEM((lat_dev, wide), BF16),
                pltpu.VMEM((wide, lat_dev), BF16),
                pltpu.VMEM((n_lay, groups, part, lat_dev), BF16),
                pltpu.VMEM((n_lay, groups, part, lat_dev), BF16),
                pltpu.VMEM((n_lat, row_dev, wide), BF16),
                pltpu.VMEM((n_lat, row_dev, wide), BF16),
                pltpu.VMEM((n_lat, row_dev, wide), BF16),
                pltpu.VMEM((groups, part, lat_dev), BF16),
                pltpu.VMEM((groups, part, lat_dev), F32),
                dma((3,)),
                dma((n_lat,)), dma((n_lat,)),
                dma((groups, n_lay)), dma((groups, n_lay)),
                dma((n_lat,)), dma((n_lat,)),
                dma((n_lat,)), dma((n_lat,)),
                dma((groups, n_lay)), dma((groups, n_lay)),
            ],
            compiler_params=pltpu.CompilerParams(collective_id=0, has_side_effects=True),
            cost_estimate=pl.CostEstimate(
                flops=8 * rows * wide * lat_dev,
                bytes_accessed=4 * wide * lat_dev,
                transcendentals=0,
            ),
        )(
            acts.reshape(row_dev, wide),
            w_enc.reshape(wide, lat_dev),
            w_dec.reshape(lat_dev, wide),
            b_enc,
            b_dec.reshape(1, wide),
        )
        lat_grad, enc_grad, dec_grad = pl.pallas_call(
            functools.partial(finish, chunks),
            out_shape=[
                jax.ShapeDtypeStruct((groups, part, lat_dev), BF16),
                jax.ShapeDtypeStruct((wide, lat_dev), BF16),
                jax.ShapeDtypeStruct((lat_dev, wide), BF16),
            ],
            in_specs=[vmem, vmem, vmem],
            out_specs=[hbm, hbm, hbm],
            scratch_shapes=[pltpu.VMEM((wide, lat_dev), BF16), dma((2 + chunks,))],
            compiler_params=pltpu.CompilerParams(vmem_limit_bytes=8 * wide * lat_dev),
            cost_estimate=pl.CostEstimate(
                flops=2 * rows * wide * lat_dev,
                bytes_accessed=4 * wide * lat_dev,
                transcendentals=0,
            ),
        )(lat_part, acts_t, dec_part)
        return (
            lat_grad.reshape(rows, lat_dev),
            enc_grad.reshape(lay_dev, width, lat_dev),
            dec_grad.reshape(lat_dev, lay_dev, width),
        )

    in_specs = (
        P(("grp", "lat"), "lay", None),
        P("lay", None, "lat"),
        P("lat", "lay", None),
        P("lat"),
        P("lay", None),
    )
    out_specs = (P("grp", "lat"), P(("grp", "lay"), None, "lat"), P("lat", ("grp", "lay"), None))
    return jax.shard_map(
        on_device, mesh=mesh, in_specs=in_specs, out_specs=out_specs, check_vma=False
    )
```

```python
import functools

import jax
import jax.numpy as jnp
from jax import lax
from jax.experimental import pallas as pl
from jax.experimental.pallas import tpu as pltpu
from jax.sharding import PartitionSpec as P

MESH = pl.DeviceIdType.MESH
F32, BF16 = jnp.float32, jnp.bfloat16


def flip(v, j):
    out, bit = v, 1
    while bit <= j:
        if j & bit:
            out = out + bit * (1 - 2 * lax.rem(lax.div(v, bit), 2))
        bit *= 2
    return out


def step(
    n_lat, n_lay, groups, acts_hbm, wenc_hbm, wdec_hbm, benc_ref, bdec_ref,
    lat_out, acts_t, dec_out,
    acts_all, wenc, wdec, wdec_t, pre_buf, back_buf, rec_mine, rec_buf, err_all, code_all, slope,
    load, acts_s, acts_r, pre_s, pre_r, rec_s, rec_r, err_s, err_r, back_s, back_r,
):
    z, l = lax.axis_index("lat"), lax.axis_index("lay")
    row_dev, wide = acts_all.shape[1:]
    rows, lat_dev = n_lat * row_dev, wenc.shape[1]
    size = n_lat // groups
    part = size * row_dev

    load_acts = pltpu.make_async_copy(acts_hbm, acts_all.at[z], load.at[0])
    load_enc = pltpu.make_async_copy(wenc_hbm, wenc, load.at[1])
    load_dec = pltpu.make_async_copy(wdec_hbm, wdec, load.at[2])
    load_acts.start()
    load_enc.start()
    load_dec.start()

    if groups > 1:
        dest = source = lambda j: flip(z, j)
    else:
        dest = lambda j: lax.rem(z + j, n_lat)
        source = lambda j: lax.rem(z + n_lat - j, n_lat)
    group = [flip(lax.div(z, size), g) if groups > 1 else 0 for g in range(groups)]

    def lay_peer(k):
        return {"lay": lax.rem(l + k, n_lay)}

    barrier = pltpu.get_barrier_semaphore()
    for j in reversed(range(1, n_lat)):
        pl.semaphore_signal(
            barrier, inc=1, device_id={"lat": dest(j)}, device_id_type=MESH
        )
    for k in range(1, n_lay):
        pl.semaphore_signal(barrier, inc=1, device_id=lay_peer(k), device_id_type=MESH)
    pl.semaphore_wait(barrier, n_lat + n_lay - 2)

    started = []

    def send(src, dst, send_sem, recv_sem, peer):
        copy = pltpu.make_async_remote_copy(
            src_ref=src, dst_ref=dst, send_sem=send_sem, recv_sem=recv_sem,
            device_id=peer, device_id_type=MESH,
        )
        copy.start()
        started.append(copy)
        return copy

    def to_lat(buf, sent, received):
        return {
            j: send(buf.at[z], buf.at[z], sent.at[j], received.at[j], {"lat": dest(j)})
            for j in range(1, n_lat)
        }

    def to_lay(buf, g, sent, received):
        block = buf.at[l, group[g]]
        return [
            send(block, block, sent.at[g, k], received.at[g, k], lay_peer(k))
            for k in range(1, n_lay)
        ]

    def arrive(copies, g):
        for j in range(g * size, (g + 1) * size):
            if j:
                copies[j].wait_recv()

    def rows_of(buf, g):
        return buf[pl.ds(group[g] * size, size)].reshape(part, wide)

    def total(buf, g):
        whole = buf[0, group[g]].astype(F32)
        for i in range(1, n_lay):
            whole += buf[i, group[g]].astype(F32)
        return whole

    load_acts.wait()
    acts_copies = to_lat(acts_all, acts_s, acts_r)
    load_enc.wait()
    pre_copies, rec_copies = {}, {}

    def encode(g):
        arrive(acts_copies, g)
        pre = jnp.dot(rows_of(acts_all, g), wenc[...], preferred_element_type=F32)
        pre_buf[l, group[g]] = pre.astype(BF16)
        pre_copies[g] = to_lay(pre_buf, g, pre_s, pre_r)

    def decode(g):
        for copy in pre_copies[g]:
            copy.wait_recv()
        x = 4.0 * (total(pre_buf, g) + benc_ref[...].reshape(1, lat_dev))
        e = jnp.exp(-jnp.abs(x))
        code = (0.25 * (jnp.maximum(x, 0.0) + jnp.log1p(e))).astype(BF16)
        rec = jnp.dot(code, wdec[...], preferred_element_type=F32).astype(BF16)
        rec_mine[pl.ds(group[g] * size, size)] = rec.reshape(size, row_dev, wide)
        for j in range(g * size, (g + 1) * size):
            if j:
                rec_copies[j] = send(
                    rec_mine.at[dest(j)], rec_buf.at[z], rec_s.at[j], rec_r.at[j],
                    {"lat": dest(j)},
                )
        code_all[group[g]] = code
        slope[group[g]] = jnp.where(x >= 0.0, 1.0, e) / (1.0 + e)

    for g in range(groups):
        encode(g)
        if g == 0:
            load_dec.wait()
    for g in [*range(1, groups), 0]:
        decode(g)
    wdec_t[...] = wdec[...].astype(F32).T.astype(BF16)
    acts_t[...] = acts_all[...].reshape(rows, wide).astype(F32).T.astype(BF16)
    code_t = code_all[...].reshape(rows, lat_dev).astype(F32).T.astype(BF16)
    err = bdec_ref[...] - acts_all[z].astype(F32) + rec_mine[z].astype(F32)
    for j in range(1, n_lat):
        rec_copies[j].wait_recv()
        err += rec_buf[source(j)].astype(F32)
    err_all[z] = err.astype(BF16)
    err_copies = to_lat(err_all, err_s, err_r)
    back_copies = {}
    for g in range(groups):
        arrive(err_copies, g)
        back = jnp.dot(rows_of(err_all, g), wdec_t[...], preferred_element_type=F32)
        back_buf[l, group[g]] = back.astype(BF16)
        back_copies[g] = to_lay(back_buf, g, back_s, back_r)
    errs = err_all[...].reshape(rows, wide)
    dec_out[...] = jnp.dot(code_t, errs, preferred_element_type=F32).astype(BF16)
    for g in range(groups):
        for copy in back_copies[g]:
            copy.wait_recv()
        lat_out[group[g]] = (total(back_buf, g) * slope[group[g]]).astype(BF16)
    for copy in started:
        copy.wait_send()


def finish(chunks, lat, acts_t, dec, lat_hbm, enc_hbm, dec_hbm, enc, sems):
    rows, lat_dev = lat.shape[0] * lat.shape[1], lat.shape[2]
    copies = [
        pltpu.make_async_copy(dec, dec_hbm, sems.at[0]),
        pltpu.make_async_copy(lat, lat_hbm, sems.at[1]),
    ]
    for copy in copies:
        copy.start()
    grad = lat[...].reshape(rows, lat_dev)
    tall = enc.shape[0] // chunks
    for c in range(chunks):
        cut = pl.ds(c * tall, tall)
        enc[cut] = jnp.dot(acts_t[cut], grad, preferred_element_type=F32).astype(BF16)
        copy = pltpu.make_async_copy(enc.at[cut], enc_hbm.at[cut], sems.at[2 + c])
        copy.start()
        copies.append(copy)
    for copy in copies:
        copy.wait()


def solution(mesh):
    n_lat, n_lay = mesh.shape["lat"], mesh.shape["lay"]

    def on_device(acts, w_enc, w_dec, b_enc, b_dec):
        row_dev, lay_dev, width = acts.shape
        lat_dev = w_enc.shape[2]
        wide, rows = lay_dev * width, n_lat * row_dev
        hbm = pl.BlockSpec(memory_space=pltpu.HBM)
        vmem = pl.BlockSpec(memory_space=pltpu.VMEM)
        dma = pltpu.SemaphoreType.DMA
        groups = 4 if n_lat & (n_lat - 1) == 0 and n_lat % 4 == 0 else 1
        part = rows // groups
        chunks = 5 if wide % 80 == 0 else 1
        lat_part, acts_t, dec_part = pl.pallas_call(
            functools.partial(step, n_lat, n_lay, groups),
            out_shape=[
                pltpu.VMEM((groups, part, lat_dev), BF16),
                pltpu.VMEM((wide, rows), BF16),
                pltpu.VMEM((lat_dev, wide), BF16),
            ],
            in_specs=[hbm, hbm, hbm, vmem, vmem],
            out_specs=[vmem, vmem, vmem],
            scratch_shapes=[
                pltpu.VMEM((n_lat, row_dev, wide), BF16),
                pltpu.VMEM((wide, lat_dev), BF16),
                pltpu.VMEM((lat_dev, wide), BF16),
                pltpu.VMEM((wide, lat_dev), BF16),
                pltpu.VMEM((n_lay, groups, part, lat_dev), BF16),
                pltpu.VMEM((n_lay, groups, part, lat_dev), BF16),
                pltpu.VMEM((n_lat, row_dev, wide), BF16),
                pltpu.VMEM((n_lat, row_dev, wide), BF16),
                pltpu.VMEM((n_lat, row_dev, wide), BF16),
                pltpu.VMEM((groups, part, lat_dev), BF16),
                pltpu.VMEM((groups, part, lat_dev), F32),
                dma((3,)),
                dma((n_lat,)), dma((n_lat,)),
                dma((groups, n_lay)), dma((groups, n_lay)),
                dma((n_lat,)), dma((n_lat,)),
                dma((n_lat,)), dma((n_lat,)),
                dma((groups, n_lay)), dma((groups, n_lay)),
            ],
            compiler_params=pltpu.CompilerParams(collective_id=0, has_side_effects=True),
            cost_estimate=pl.CostEstimate(
                flops=8 * rows * wide * lat_dev,
                bytes_accessed=4 * wide * lat_dev,
                transcendentals=0,
            ),
        )(
            acts.reshape(row_dev, wide),
            w_enc.reshape(wide, lat_dev),
            w_dec.reshape(lat_dev, wide),
            b_enc,
            b_dec.reshape(1, wide),
        )
        lat_grad, enc_grad, dec_grad = pl.pallas_call(
            functools.partial(finish, chunks),
            out_shape=[
                jax.ShapeDtypeStruct((groups, part, lat_dev), BF16),
                jax.ShapeDtypeStruct((wide, lat_dev), BF16),
                jax.ShapeDtypeStruct((lat_dev, wide), BF16),
            ],
            in_specs=[vmem, vmem, vmem],
            out_specs=[hbm, hbm, hbm],
            scratch_shapes=[pltpu.VMEM((wide, lat_dev), BF16), dma((2 + chunks,))],
            compiler_params=pltpu.CompilerParams(vmem_limit_bytes=8 * wide * lat_dev),
            cost_estimate=pl.CostEstimate(
                flops=2 * rows * wide * lat_dev,
                bytes_accessed=4 * wide * lat_dev,
                transcendentals=0,
            ),
        )(lat_part, acts_t, dec_part)
        return (
            lat_grad.reshape(rows, lat_dev),
            enc_grad.reshape(lay_dev, width, lat_dev),
            dec_grad.reshape(lat_dev, lay_dev, width),
        )

    in_specs = (
        P(("grp", "lat"), "lay", None),
        P("lay", None, "lat"),
        P("lat", "lay", None),
        P("lat"),
        P("lay", None),
    )
    out_specs = (P("grp", "lat"), P(("grp", "lay"), None, "lat"), P("lat", ("grp", "lay"), None))
    return jax.shard_map(
        on_device, mesh=mesh, in_specs=in_specs, out_specs=out_specs, check_vma=False
    )
```
